512 devices in a mesh: subj: 2 (over y), row: 16 (over x, core), col: 16 (over z).
Axes of the slice: x: 8, y: 2, z: 16, core: 2. Of those that a mesh axis runs over, the one named last changes fastest.
The devices are a block of a 8x8x16 slice.
Arguments:
- series: float32 [800, 65536], P(None, ('subj', 'row', 'col')), parts along dimension 1, as said below
- keep_mask: int32 [512, 256], P(('subj', 'row'), 'col'), parts along dimension 0, may hold values from 0 to 1, as said below
- row_owner: int32 [512], P('subj'), parts along dimension 0, may hold values from 0 to 15, as said below
Outputs:
- owned_tiles: bfloat16 [32, 16, 96, 128, 128], P(('subj', 'row'), 'col'), parts along dimension 0
- owned_ids: int32 [32, 16, 96], P(('subj', 'row'), 'col'), parts along dimension 0
The draws below stay inside these ranges and needn't reach their ends.
There are 2 independent parts, one for each index of `subj`. The reference program is written for one: setup_inputs(seed, part) draws one part's arguments, and reference() takes and returns one part's arrays. A program takes and returns all parts, laid end to end along the dimension named above; each array names one. Nothing has to cross between parts.
Inputs may be any that keep to these rules, and one draw needn't show every extreme that they name: Each voxel's series varies over time. `keep_mask`: of the 16 tiles that one tile row has in one column block, at most 6 are kept; in every draw one owner keeps exactly 6 in each of its tile rows in some column block. `row_owner`: the 16 tile rows of a row block have 16 different owners, and every owner holds 16 tile rows, from 16 different row blocks.
All inputs are finite; a program needn't handle non-finite values.
Results may differ from the reference program's by a relative error of at most 0.0042.
Values may be sent and summed in bfloat16 or wider, within the bound.
No kernel may reach another device: no remote copies, remote signals or barrier semaphores. Data moves between devices by JAX's collectives and lax.ppermute only.
A program may use at most 64 MiB of HBM per device.

```python
import math
import jax
import jax.numpy as jnp
from jax import lax

TRS = 800
TILE = 128
CH = 128
NVOX = 32768
NTILES = 256
RT = 16
CT = 16
CAP = 6
RCAP = 96
N_ROW = 16
N_COL = 16


latent_count = 128


def draw_series(key, part):
    subkeys = jax.random.split(key, 6)
    latent = jax.random.normal(subkeys[0], (TRS, latent_count), jnp.float32)
    loadings = 1.2 / math.sqrt(latent_count) * jax.random.normal(subkeys[1], (latent_count, NVOX), jnp.float32)
    tr_scale = jnp.exp(jax.random.uniform(subkeys[4], (TRS, 1), jnp.float32, 0.0, math.log(1.2)))
    offset = jax.random.uniform(subkeys[5], (1, NVOX), jnp.float32, -5.0, 5.0)
    noise_part = jax.random.normal(subkeys[2], (TRS, NVOX), jnp.float32)
    vox_scale = jnp.exp(jax.random.uniform(subkeys[3], (1, NVOX), jnp.float32, 0.0, math.log(10.0)))
    signal = jnp.dot(latent, loadings) + noise_part
    return (offset + vox_scale * tr_scale * signal).astype(jnp.float32)


def routing(key):
    base_key = jax.random.fold_in(key, 7)
    row_blocks = NTILES // RT
    col_blocks = NTILES // CT
    owner_order = jax.random.permutation(jax.random.fold_in(base_key, 1), row_blocks)
    shifts = jax.vmap(lambda subkey: jax.random.permutation(subkey, RT))(jax.random.split(jax.random.fold_in(base_key, 2), row_blocks))
    block_ids = jnp.arange(row_blocks, dtype=jnp.int32)[:, None]
    owners = owner_order[(block_ids + shifts) % row_blocks].reshape(NTILES).astype(jnp.int32)
    load_level = jax.random.randint(jax.random.fold_in(base_key, 3), (row_blocks,), 0, 3)
    slot_draw = jax.random.randint(jax.random.fold_in(base_key, 4), (NTILES, col_blocks), 0, CAP + 1)
    slot_limit = jnp.minimum(CAP, slot_draw * (1 + load_level[owners])[:, None] // 2)
    forced = (owners == owner_order[0])[:, None] & (jnp.arange(col_blocks) == 0)[None, :]
    slot_limit = jnp.where(forced, CAP, slot_limit)
    tile_ranks = jax.vmap(lambda subkey: jax.random.permutation(subkey, CT))(jax.random.split(jax.random.fold_in(base_key, 5), NTILES * col_blocks))
    tile_ranks = tile_ranks.reshape(NTILES, col_blocks, CT)
    kept = (tile_ranks < slot_limit[:, :, None]).astype(jnp.int32).reshape(NTILES, NTILES)
    return (kept, owners)


def draw_keep_mask(key, part):
    kept, owners = routing(key)
    return kept


def draw_row_owner(key, part):
    kept, owners = routing(key)
    return owners


def setup_inputs(seed: int = 0, part: int = 0) -> dict:
    key_of = jax.random.split(jax.random.key(seed), 4)
    part_keys = jax.random.split(jax.random.fold_in(key_of[3], part), 4)
    series = draw_series(jax.random.fold_in(jax.random.fold_in(key_of[3], part), 71), part)
    keep_mask = draw_keep_mask(jax.random.fold_in(jax.random.fold_in(key_of[3], part), 71), part)
    row_owner = draw_row_owner(jax.random.fold_in(jax.random.fold_in(key_of[3], part), 71), part)
    return {"series": series, "keep_mask": keep_mask, "row_owner": row_owner}


epsilon = 1e-05

def reference(series, keep_mask, row_owner):
    average = lax.optimization_barrier(jnp.mean(series, axis=0, keepdims=True))
    centred = series - average
    spread = lax.optimization_barrier(jnp.mean(centred * centred, axis=0, keepdims=True))
    scored = (centred * lax.rsqrt(spread + epsilon)).astype(jnp.bfloat16)
    reordered = scored.reshape(TRS, N_ROW, N_COL, CH).transpose(0, 2, 1, 3).reshape(TRS, NVOX)
    row_tiles = scored.reshape(TRS, NTILES, TILE)
    col_tiles = reordered.reshape(TRS, NTILES, TILE)
    positions = jnp.arange(NTILES * CT, dtype=jnp.int32)
    slot_index = jnp.arange(RCAP, dtype=jnp.int32)

    def one_group(group_index):
        target = group_index // N_COL
        column_block = group_index % N_COL
        block_keep = lax.dynamic_slice_in_dim(keep_mask, (column_block * CT).astype(jnp.int32), CT, 1)
        owned = (row_owner == target).astype(jnp.int32)
        keep_flags = (block_keep * owned[:, None]).reshape(NTILES * CT)
        running = jnp.cumsum(keep_flags)
        slot_hit = (keep_flags[None, :] == 1) & (running[None, :] == slot_index[:, None] + 1)
        picked = lax.optimization_barrier(jnp.sum(jnp.where(slot_hit, positions[None, :], 0), axis=1)).astype(jnp.int32)
        present = running[-1] > slot_index
        row_ids = (picked // CT).astype(jnp.int32)
        col_ids = (column_block * CT + picked % CT).astype(jnp.int32)
        left_tiles = jnp.take(row_tiles, row_ids, axis=1).astype(jnp.float32)
        right_tiles = jnp.take(col_tiles, col_ids, axis=1).astype(jnp.float32)
        products = jnp.einsum('tsa,tsb->sab', left_tiles, right_tiles) * (1.0 / TRS)
        slot_tiles = jnp.where(present[:, None, None], products, 0.0).astype(jnp.bfloat16)
        slot_ids = jnp.where(present, row_ids * NTILES + col_ids, -1).astype(jnp.int32)
        return (slot_tiles, slot_ids)
    slot_tiles, slot_ids = lax.map(one_group, jnp.arange(N_ROW * N_COL, dtype=jnp.int32))
    return (slot_tiles.reshape(N_ROW, N_COL, RCAP, TILE, TILE), slot_ids.reshape(N_ROW, N_COL, RCAP))
```

```python
import functools

import jax
import jax.numpy as jnp
from jax import lax
from jax.experimental import pallas as pl
from jax.experimental.pallas import tpu as pltpu
from jax.sharding import PartitionSpec as P

EPS = 1e-05
LANES = 128
ALIGN = 8
COPIES = 2
VMEM_LIMIT = 24 * 2**20

VMEM = pl.BlockSpec(memory_space=pltpu.VMEM)
SMEM = pl.BlockSpec(memory_space=pltpu.SMEM)


def score_kernel(series_ref, scored_ref, chunks_ref):
    frames = series_ref.shape[0]
    _, sub, padded = chunks_ref.shape
    groups = LANES // sub
    x = series_ref[...]
    centred = x - jnp.sum(x, axis=0, keepdims=True) * (1.0 / frames)
    spread = jnp.sum(centred * centred, axis=0, keepdims=True) * (1.0 / frames)
    z = centred * lax.rsqrt(spread + EPS)
    scored_ref[...] = z.astype(jnp.bfloat16)
    for b in range(padded // LANES):
        rows = min(LANES, frames - b * LANES)
        part = z[b * LANES : b * LANES + rows]
        if rows < LANES:
            part = jnp.concatenate([part, jnp.zeros((LANES - rows, LANES), jnp.float32)], axis=0)
        flipped = part.T.astype(jnp.bfloat16)
        flipped = flipped.reshape(groups, sub, LANES)
        for copy in range(COPIES):
            at = copy * groups
            chunks_ref[at : at + groups, :, b * LANES : (b + 1) * LANES] = flipped


def route_kernel(frames, where_ref, owner_ref, chunks_ref, keep_ref, out_ref):
    n = chunks_ref.shape[0]
    padded = chunks_ref.shape[2]
    last = padded - LANES
    gap = frames - last
    flags = keep_ref[...].astype(jnp.float32)
    flags = jnp.concatenate(
        [
            jnp.zeros((n, gap), jnp.float32),
            flags,
            jnp.zeros((n, LANES - gap - flags.shape[1]), jnp.float32),
        ],
        axis=1,
    )
    base = where_ref[0] * n
    for k in range(n):
        owner = owner_ref[base + k]
        out_ref[owner, :, :last] = chunks_ref[k, :, :last]
        tail = chunks_ref[k, :, last:].astype(jnp.float32) + flags[k : k + 1]
        out_ref[owner, :, last:] = tail.astype(jnp.bfloat16)


def pack_kernel(frames, where_ref, got_ref, owner_ref, packed_ref, code_ref, ids_ref):
    n, sub, padded = got_ref.shape
    rows = n * sub
    last = padded - LANES
    gap = frames - last
    for b in range(last // LANES):
        block = got_ref[:, :, b * LANES : (b + 1) * LANES]
        packed_ref[b * rows : (b + 1) * rows, :] = block.reshape(rows, LANES)
    tail = got_ref[:, :, last:].reshape(rows, LANES)
    per = LANES // gap
    depth = rows // per
    packed_ref[last // LANES * rows :, :] = jnp.concatenate(
        [tail[q * depth : (q + 1) * depth, :gap] for q in range(per)], axis=1
    )
    me = where_ref[0]
    block = where_ref[1]
    flags = got_ref[:, 0, last:].astype(jnp.float32)[:, gap : gap + n]
    r_of = lax.broadcasted_iota(jnp.int32, (n, n), 0)
    k_of = lax.broadcasted_iota(jnp.int32, (n, n), 1)
    upper = (r_of <= k_of).astype(jnp.float32)
    lower = (r_of > k_of).astype(jnp.float32)
    within = jnp.dot(flags, upper, preferred_element_type=jnp.float32)
    before = jnp.sum(
        jnp.dot(lower, flags, preferred_element_type=jnp.float32), axis=1, keepdims=True
    )
    place = (before + within - 1.0).astype(jnp.int32)
    place = jnp.where(flags > 0.5, place, -1)
    picked = jnp.sum(jnp.where(owner_ref[...] == me, k_of, 0), axis=1, keepdims=True)
    lane = lax.broadcasted_iota(jnp.int32, (n, LANES), 1)
    row = lax.broadcasted_iota(jnp.int32, (n, LANES), 0)
    tiles = n * n
    found = jnp.zeros((n, LANES), jnp.int32)
    code = jnp.zeros((n, LANES), jnp.int32)
    ids = jnp.zeros((n, LANES), jnp.int32)
    for j in range(n):
        hit = place[:, j : j + 1] == lane
        found = found + hit.astype(jnp.int32)
        code = code + jnp.where(hit, j * rows + row * sub, 0)
        ids = ids + jnp.where(hit, (row * n + picked) * tiles + block * n + j, 0)
    found = jnp.sum(found, axis=0, keepdims=True)
    code = jnp.where(found > 0, jnp.sum(code, axis=0, keepdims=True), n * rows)
    ids = jnp.where(found > 0, jnp.sum(ids, axis=0, keepdims=True), -1)
    code_ref[...] = jnp.broadcast_to(code, code_ref.shape)
    ids_ref[0] = ids[:, : ids_ref.shape[2]]


def strip_kernel(scale, frames, offset, where_ref, code_ref, part, cols_ref, _, out_ref, prod_ref):
    n = cols_ref.shape[0]
    slots = out_ref.shape[0]
    rows = prod_ref.shape[0] // (n + 1)
    sub = rows // n
    groups = LANES // sub
    last = frames // LANES
    gap = frames - last * LANES
    pieces = [part[b * rows : (b + 1) * rows, :] for b in range(last)]
    tail = part[last * rows :, :]
    pieces.append(jnp.concatenate([tail[:, q : q + gap] for q in range(0, LANES, gap)], axis=0))
    left = jnp.concatenate(pieces, axis=1)
    prod_ref[n * rows : n * rows + sub, :] = jnp.zeros((sub, LANES), jnp.float32)
    for g in range(n // 2):
        pair = jnp.concatenate([cols_ref[2 * g], cols_ref[2 * g + 1]], axis=1)
        prod = jnp.dot(left, pair, preferred_element_type=jnp.float32)
        for h in range(2):
            at = (2 * g + h) * rows
            prod_ref[at : at + rows, :] = prod[:, h * LANES : (h + 1) * LANES]
    group = lax.rem(where_ref[1] + (offset + groups), groups)
    into = pl.ds(pl.multiple_of(group * sub, sub), sub)
    for s in range(slots):
        strip = prod_ref[pl.ds(pl.multiple_of(code_ref[0, s], sub), sub), :]
        out_ref[s, into, :] = (strip * scale).astype(jnp.bfloat16)


def in_vmem(x):
    return pltpu.with_memory_space_constraint(x, pltpu.VMEM)


def strips(part, offset, where, code, cols, out, scale):
    n, frames, _ = cols.shape
    rows = part.shape[0] * LANES // frames
    return pl.pallas_call(
        functools.partial(strip_kernel, scale, frames, offset),
        out_shape=pltpu.VMEM(out.shape, out.dtype),
        in_specs=[SMEM, SMEM, VMEM, VMEM, VMEM],
        out_specs=VMEM,
        input_output_aliases={4: 0},
        scratch_shapes=[pltpu.VMEM(((n + 1) * rows, LANES), jnp.float32)],
        compiler_params=pltpu.CompilerParams(vmem_limit_bytes=VMEM_LIMIT),
        name="strips",
    )(where, code, in_vmem(part), in_vmem(cols), in_vmem(out))


def alloc(shape, dtype):
    def nothing(out_ref):
        pass

    return pl.pallas_call(
        nothing,
        out_shape=pltpu.VMEM(shape, dtype),
        out_specs=VMEM,
        compiler_params=pltpu.CompilerParams(vmem_limit_bytes=VMEM_LIMIT),
        name="alloc",
    )()


def shards(series, keep_mask, row_owner):
    frames = series.shape[0]
    n_row = lax.axis_size("row")
    n_col = lax.axis_size("col")
    row_count, col_count = keep_mask.shape
    slot_limit = max(2, 3 * col_count // 8)
    capacity = row_count * slot_limit
    padded = -(-frames // LANES) * LANES
    groups = n_col // COPIES
    sub = LANES // groups
    my_row = lax.axis_index("row")
    my_col = lax.axis_index("col")
    where = jnp.stack([my_row, my_col]).astype(jnp.int32)
    bf16 = jnp.bfloat16
    sds = jax.ShapeDtypeStruct

    scored, chunks = pl.pallas_call(
        score_kernel,
        out_shape=(sds((frames, LANES), bf16), sds((n_col, sub, padded), bf16)),
        in_specs=[VMEM],
        out_specs=(VMEM, VMEM),
        name="score",
    )(series)

    mixed = lax.all_to_all(chunks, "col", 0, 0, tiled=True)
    routed = pl.pallas_call(
        functools.partial(route_kernel, frames),
        out_shape=sds((n_row, sub, padded), bf16),
        in_specs=[SMEM, SMEM, VMEM, VMEM],
        out_specs=VMEM,
        name="route",
    )(where, row_owner, mixed, keep_mask)
    got = lax.all_to_all(routed, "row", 0, 0, tiled=True)
    packed, code, ids = pl.pallas_call(
        functools.partial(pack_kernel, frames),
        out_shape=(
            sds((frames * n_row * sub // LANES, LANES), bf16),
            sds((ALIGN, LANES), jnp.int32),
            sds((1, 1, capacity), jnp.int32),
        ),
        in_specs=[SMEM, VMEM, VMEM],
        out_specs=(VMEM, VMEM, VMEM),
        name="pack",
    )(where, got, row_owner.reshape(n_row, row_count))

    cols = lax.all_gather(scored, "row", axis=0, tiled=False)

    out = alloc((capacity, LANES, LANES), bf16)
    cols = in_vmem(cols)
    fill = functools.partial(strips, where=where, code=code, cols=cols, scale=1.0 / frames)
    right = [(i, (i + 1) % n_col) for i in range(n_col)]
    left = [(i, (i - 1) % n_col) for i in range(n_col)]
    half = groups // 2
    a = lax.ppermute(packed, "col", right)
    b = lax.ppermute(packed, "col", left)
    out = fill(packed, 0, out=out)
    for step in range(1, half + 1):
        here, there = a, b
        if step < half:
            here, out = lax.optimization_barrier((here, out))
            a = lax.ppermute(here, "col", right)
        out = fill(here, -step, out=out)
        if step < half:
            if step < half - 1:
                there, out = lax.optimization_barrier((there, out))
                b = lax.ppermute(there, "col", left)
            out = fill(there, step, out=out)
    return out.reshape(1, 1, capacity, LANES, LANES), ids


def solution(mesh):
    in_specs = (P(None, ("subj", "row", "col")), P(("subj", "row"), "col"), P("subj"))
    out_specs = (P(("subj", "row"), "col", None, None, None), P(("subj", "row"), "col", None))
    return jax.shard_map(shards, mesh=mesh, in_specs=in_specs, out_specs=out_specs, check_vma=False)
```

```python
import functools

import jax
import jax.numpy as jnp
from jax import lax
from jax.experimental import pallas as pl
from jax.experimental.pallas import tpu as pltpu
from jax.sharding import PartitionSpec as P


EPS = 1e-05
LANES = 128
ALIGN = 8
COPIES = 2
VMEM_LIMIT = 24 * 2**20

VMEM = pl.BlockSpec(memory_space=pltpu.VMEM)
SMEM = pl.BlockSpec(memory_space=pltpu.SMEM)


def score_kernel(series_ref, scored_ref, chunks_ref):
    frames = series_ref.shape[0]
    _, sub, padded = chunks_ref.shape
    groups = LANES // sub
    x = series_ref[...]
    centred = x - jnp.sum(x, axis=0, keepdims=True) * (1.0 / frames)
    spread = jnp.sum(centred * centred, axis=0, keepdims=True) * (1.0 / frames)
    z = centred * lax.rsqrt(spread + EPS)
    scored_ref[...] = z.astype(jnp.bfloat16)
    for b in range(padded // LANES):
        rows = min(LANES, frames - b * LANES)
        part = z[b * LANES : b * LANES + rows]
        if rows < LANES:
            part = jnp.concatenate([part, jnp.zeros((LANES - rows, LANES), jnp.float32)], axis=0)
        flipped = part.T.astype(jnp.bfloat16)
        flipped = flipped.reshape(groups, sub, LANES)
        for copy in range(COPIES):
            at = copy * groups
            chunks_ref[at : at + groups, :, b * LANES : (b + 1) * LANES] = flipped


def route_kernel(frames, where_ref, owner_ref, chunks_ref, keep_ref, out_ref):
    n = chunks_ref.shape[0]
    padded = chunks_ref.shape[2]
    last = padded - LANES
    gap = frames - last
    flags = keep_ref[...].astype(jnp.float32)
    flags = jnp.concatenate(
        [
            jnp.zeros((n, gap), jnp.float32),
            flags,
            jnp.zeros((n, LANES - gap - flags.shape[1]), jnp.float32),
        ],
        axis=1,
    )
    base = where_ref[0] * n
    for k in range(n):
        owner = owner_ref[base + k]
        out_ref[owner, :, :last] = chunks_ref[k, :, :last]
        tail = chunks_ref[k, :, last:].astype(jnp.float32) + flags[k : k + 1]
        out_ref[owner, :, last:] = tail.astype(jnp.bfloat16)


def pack_kernel(frames, where_ref, got_ref, owner_ref, packed_ref, code_ref, ids_ref):
    n, sub, padded = got_ref.shape
    rows = n * sub
    last = padded - LANES
    gap = frames - last
    blocks = [
        got_ref[:, :, b : b + LANES].reshape(rows, LANES) for b in range(0, last, LANES)
    ]
    tail = got_ref[:, :, last:].reshape(rows, LANES)
    per = LANES // gap
    depth = rows // per
    tail = jnp.concatenate([tail[q * depth : (q + 1) * depth, :gap] for q in range(per)], axis=1)
    for b, block in enumerate(blocks):
        packed_ref[b * rows : (b + 1) * rows, :] = block
    packed_ref[len(blocks) * rows :, :] = tail
    me = where_ref[0]
    block = where_ref[1]
    flags = got_ref[:, 0, last:].astype(jnp.float32)[:, gap : gap + n]
    r_of = lax.broadcasted_iota(jnp.int32, (n, n), 0)
    k_of = lax.broadcasted_iota(jnp.int32, (n, n), 1)
    upper = (r_of <= k_of).astype(jnp.float32)
    lower = (r_of > k_of).astype(jnp.float32)
    within = jnp.dot(flags, upper, preferred_element_type=jnp.float32)
    before = jnp.sum(
        jnp.dot(lower, flags, preferred_element_type=jnp.float32), axis=1, keepdims=True
    )
    place = (before + within - 1.0).astype(jnp.int32)
    place = jnp.where(flags > 0.5, place, -1)
    picked = jnp.sum(jnp.where(owner_ref[...] == me, k_of, 0), axis=1, keepdims=True)
    lane = lax.broadcasted_iota(jnp.int32, (n, LANES), 1)
    row = lax.broadcasted_iota(jnp.int32, (n, LANES), 0)
    tiles = n * n
    found = jnp.zeros((n, LANES), jnp.int32)
    code = jnp.zeros((n, LANES), jnp.int32)
    ids = jnp.zeros((n, LANES), jnp.int32)
    for j in range(n):
        hit = place[:, j : j + 1] == lane
        found = found + hit.astype(jnp.int32)
        code = code + jnp.where(hit, j * rows + row * sub, 0)
        ids = ids + jnp.where(hit, (row * n + picked) * tiles + block * n + j, 0)
    found = jnp.sum(found, axis=0, keepdims=True)
    code = jnp.where(found > 0, jnp.sum(code, axis=0, keepdims=True), n * rows)
    ids = jnp.where(found > 0, jnp.sum(ids, axis=0, keepdims=True), -1)
    code_ref[...] = jnp.broadcast_to(code, code_ref.shape)
    ids_ref[0] = ids[:, : ids_ref.shape[2]]


def strip_kernel(
    scale, frames, offset, where_ref, code_ref, part, mine_ref, other_ref, _, out_ref, prod_ref
):
    chips = mine_ref.shape[0]
    n = 2 * chips
    slots = out_ref.shape[0]
    rows = prod_ref.shape[0] // (n + 1)
    sub = rows // n
    groups = LANES // sub
    last = frames // LANES
    gap = frames - last * LANES
    pieces = [part[b * rows : (b + 1) * rows, :] for b in range(last)]
    tail = part[last * rows :, :]
    pieces.append(jnp.concatenate([tail[:, q : q + gap] for q in range(0, LANES, gap)], axis=0))
    left = jnp.concatenate(pieces, axis=1)
    prod_ref[n * rows : n * rows + sub, :] = jnp.zeros((sub, LANES), jnp.float32)
    chip, core = where_ref[0] // 2, where_ref[0] % 2
    for m, away in enumerate(aways(chips)):
        pair = jnp.concatenate([mine_ref[m], other_ref[m]], axis=1)
        prod = jnp.dot(left, pair, preferred_element_type=jnp.float32)
        first = lax.rem(chip + (away + chips), chips) * 2
        for h, j in enumerate((first + core, first + 1 - core)):
            at = pl.multiple_of(j * rows, rows)
            prod_ref[pl.ds(at, rows), :] = prod[:, h * LANES : (h + 1) * LANES]
    group = lax.rem(where_ref[1] + (offset + groups), groups)
    into = pl.ds(pl.multiple_of(group * sub, sub), sub)
    for s in range(slots):
        strip = prod_ref[pl.ds(pl.multiple_of(code_ref[0, s], sub), sub), :]
        out_ref[s, into, :] = (strip * scale).astype(jnp.bfloat16)


def in_vmem(x):
    return pltpu.with_memory_space_constraint(x, pltpu.VMEM)


def in_hbm(x):
    return pltpu.with_memory_space_constraint(x, pltpu.HBM)


def strips(part, offset, where, code, mine, other, out, scale):
    chips, frames, _ = mine.shape
    rows = part.shape[0] * LANES // frames
    return pl.pallas_call(
        functools.partial(strip_kernel, scale, frames, offset),
        out_shape=pltpu.VMEM(out.shape, out.dtype),
        in_specs=[SMEM, SMEM] + [VMEM] * 4,
        out_specs=VMEM,
        input_output_aliases={5: 0},
        scratch_shapes=[pltpu.VMEM(((2 * chips + 1) * rows, LANES), jnp.float32)],
        compiler_params=pltpu.CompilerParams(vmem_limit_bytes=VMEM_LIMIT),
        name="strips",
    )(where, code, in_vmem(part), in_vmem(mine), in_vmem(other), in_vmem(out))


def aways(chips):
    return [-m for m in range(chips // 2 + 1)] + list(range(1, (chips + 1) // 2))


def stack_kernel(*refs):
    *parts, out_ref = refs
    for m, part in enumerate(parts):
        out_ref[m] = part[...]


def alloc(shape, dtype):
    def nothing(out_ref):
        pass

    return pl.pallas_call(
        nothing,
        out_shape=pltpu.VMEM(shape, dtype),
        out_specs=VMEM,
        compiler_params=pltpu.CompilerParams(vmem_limit_bytes=VMEM_LIMIT),
        name="alloc",
    )()


def gathered(series, keep_mask, row_owner):
    frames = series.shape[0]
    n_row = lax.axis_size("row")
    n_col = lax.axis_size("col")
    row_count, col_count = keep_mask.shape
    slot_limit = max(2, 3 * col_count // 8)
    capacity = row_count * slot_limit
    padded = -(-frames // LANES) * LANES
    groups = n_col // COPIES
    sub = LANES // groups
    my_row = lax.axis_index("row")
    my_col = lax.axis_index("col")
    where = jnp.stack([my_row, my_col]).astype(jnp.int32)
    bf16 = jnp.bfloat16
    sds = jax.ShapeDtypeStruct

    small = pltpu.CompilerParams(vmem_limit_bytes=VMEM_LIMIT)
    scored, chunks = pl.pallas_call(
        score_kernel,
        out_shape=(pltpu.VMEM((frames, LANES), bf16), pltpu.VMEM((n_col, sub, padded), bf16)),
        in_specs=[VMEM],
        out_specs=(VMEM, VMEM),
        compiler_params=small,
        name="score",
    )(series)

    right = [(i, (i + 2) % n_row) for i in range(n_row)]
    left = [(i, (i - 2) % n_row) for i in range(n_row)]
    swap = [(i, i ^ 1) for i in range(n_row)]
    chips = n_row // 2
    mixed = lax.all_to_all(chunks, "col", 0, 0, tiled=True)
    hops = {"right": [scored], "left": [scored]}

    def hop(way, perm):
        hops[way].append(lax.ppermute(hops[way][-1], "row", perm))

    for step in range(1, chips // 2):
        hop("right", right)
        if step < chips // 2 - 1:
            hop("left", left)
    routed = pl.pallas_call(
        functools.partial(route_kernel, frames),
        out_shape=pltpu.VMEM((n_row, sub, padded), bf16),
        in_specs=[SMEM, SMEM, VMEM, VMEM],
        out_specs=VMEM,
        compiler_params=small,
        name="route",
    )(where, in_hbm(row_owner), in_vmem(mixed), in_hbm(keep_mask))
    got = lax.all_to_all(routed, "row", 0, 0, tiled=True)
    long = frames * n_row * sub // LANES
    packed, code, ids = pl.pallas_call(
        functools.partial(pack_kernel, frames),
        out_shape=(
            pltpu.VMEM((long, LANES), bf16),
            sds((ALIGN, LANES), jnp.int32),
            sds((1, 1, capacity), jnp.int32),
        ),
        in_specs=[SMEM, VMEM, VMEM],
        out_specs=(VMEM,) * 3,
        compiler_params=small,
        name="pack",
    )(where, in_vmem(got), row_owner.reshape(n_row, row_count))

    ring_right = [(i, (i + 1) % n_col) for i in range(n_col)]
    ring_left = [(i, (i - 1) % n_col) for i in range(n_col)]
    a = lax.ppermute(packed, "col", ring_right)
    b = lax.ppermute(packed, "col", ring_left)

    hops["right"][-1], hops["left"][-1], packed = lax.optimization_barrier(
        (hops["right"][-1], hops["left"][-1], packed)
    )
    hop("right", right)
    hop("left", left)
    mine = pl.pallas_call(
        stack_kernel,
        out_shape=pltpu.VMEM((chips, frames, LANES), bf16),
        in_specs=[VMEM] * chips,
        out_specs=VMEM,
        compiler_params=small,
        name="stack",
    )(*map(in_vmem, hops["right"] + hops["left"][1:]))
    other = lax.ppermute(mine, "row", swap)

    out = alloc((capacity, LANES, LANES), bf16)
    fill = functools.partial(
        strips, where=where, code=code, mine=mine, other=other, scale=1.0 / frames
    )
    half = groups // 2
    waiting = [(packed, 0), (a, -1), (b, 1)]
    for step in range(2, half + 1):
        if step > 2:
            out = fill(*waiting.pop(0), out=out)
            a, out = lax.optimization_barrier((a, out))
        a = lax.ppermute(a, "col", ring_right)
        waiting.append((a, -step))
        if step < half:
            if step > 2:
                out = fill(*waiting.pop(0), out=out)
                b, out = lax.optimization_barrier((b, out))
            b = lax.ppermute(b, "col", ring_left)
            waiting.append((b, step))
    for part, offset in waiting:
        out = fill(part, offset, out=out)
    return out.reshape(1, 1, capacity, LANES, LANES), ids


def solution(mesh):
    in_specs = (P(None, ("subj", "row", "col")), P(("subj", "row"), "col"), P("subj"))
    out_specs = (P(("subj", "row"), "col", None, None, None), P(("subj", "row"), "col", None))
    return jax.shard_map(
        gathered, mesh=mesh, in_specs=in_specs, out_specs=out_specs, check_vma=False
    )
```

```python
import functools

import jax
import jax.numpy as jnp
from jax import lax
from jax.experimental import pallas as pl
from jax.experimental.pallas import tpu as pltpu
from jax.sharding import PartitionSpec as P


EPS = 1e-05
LANES = 128
ALIGN = 8
COPIES = 2
VMEM_LIMIT = 24 * 2**20

VMEM = pl.BlockSpec(memory_space=pltpu.VMEM)
SMEM = pl.BlockSpec(memory_space=pltpu.SMEM)


def score_kernel(series_ref, scored_ref, chunks_ref):
    frames = series_ref.shape[0]
    _, sub, padded = chunks_ref.shape
    groups = LANES // sub
    x = series_ref[...]
    centred = x - jnp.sum(x, axis=0, keepdims=True) * (1.0 / frames)
    spread = jnp.sum(centred * centred, axis=0, keepdims=True) * (1.0 / frames)
    z = centred * lax.rsqrt(spread + EPS)
    scored_ref[...] = z.astype(jnp.bfloat16)
    for b in range(padded // LANES):
        rows = min(LANES, frames - b * LANES)
        part = z[b * LANES : b * LANES + rows]
        if rows < LANES:
            part = jnp.concatenate([part, jnp.zeros((LANES - rows, LANES), jnp.float32)], axis=0)
        flipped = part.T.astype(jnp.bfloat16)
        flipped = flipped.reshape(groups, sub, LANES)
        for copy in range(COPIES):
            at = copy * groups
            chunks_ref[at : at + groups, :, b * LANES : (b + 1) * LANES] = flipped


def route_kernel(frames, owner_ref, chunks_ref, keep_ref, out_ref):
    n = chunks_ref.shape[0]
    padded = chunks_ref.shape[2]
    last = padded - LANES
    gap = frames - last
    flags = keep_ref[...].astype(jnp.float32)
    flags = jnp.concatenate(
        [
            jnp.zeros((n, gap), jnp.float32),
            flags,
            jnp.zeros((n, LANES - gap - flags.shape[1]), jnp.float32),
        ],
        axis=1,
    )
    base = lax.axis_index("row") * n
    for k in range(n):
        owner = owner_ref[base + k]
        out_ref[owner, :, :last] = chunks_ref[k, :, :last]
        tail = chunks_ref[k, :, last:].astype(jnp.float32) + flags[k : k + 1]
        out_ref[owner, :, last:] = tail.astype(jnp.bfloat16)


def pack_kernel(frames, got_ref, packed_ref):
    n, sub, padded = got_ref.shape
    rows = n * sub
    last = padded - LANES
    gap = frames - last
    blocks = [
        got_ref[:, :, b : b + LANES].reshape(rows, LANES) for b in range(0, last, LANES)
    ]
    tail = got_ref[:, :, last:].reshape(rows, LANES)
    per = LANES // gap
    depth = rows // per
    tail = jnp.concatenate([tail[q * depth : (q + 1) * depth, :gap] for q in range(per)], axis=1)
    for b, block in enumerate(blocks):
        packed_ref[b * rows : (b + 1) * rows, :] = block
    packed_ref[len(blocks) * rows :, :] = tail


def list_kernel(frames, got_ref, owner_ref, code_ref, ids_ref):
    n, sub, padded = got_ref.shape
    rows = n * sub
    last = padded - LANES
    gap = frames - last
    me = lax.axis_index("row")
    block = lax.axis_index("col")
    flags = got_ref[:, 0, last:].astype(jnp.float32)[:, gap : gap + n]
    r_of = lax.broadcasted_iota(jnp.int32, (n, n), 0)
    k_of = lax.broadcasted_iota(jnp.int32, (n, n), 1)
    upper = (r_of <= k_of).astype(jnp.float32)
    lower = (r_of > k_of).astype(jnp.float32)
    within = jnp.dot(flags, upper, preferred_element_type=jnp.float32)
    before = jnp.sum(
        jnp.dot(lower, flags, preferred_element_type=jnp.float32), axis=1, keepdims=True
    )
    place = (before + within - 1.0).astype(jnp.int32)
    place = jnp.where(flags > 0.5, place, -1)
    picked = jnp.sum(jnp.where(owner_ref[...] == me, k_of, 0), axis=1, keepdims=True)
    lane = lax.broadcasted_iota(jnp.int32, (n, LANES), 1)
    row = lax.broadcasted_iota(jnp.int32, (n, LANES), 0)
    tiles = n * n
    found = jnp.zeros((n, LANES), jnp.int32)
    code = jnp.zeros((n, LANES), jnp.int32)
    ids = jnp.zeros((n, LANES), jnp.int32)
    for j in range(n):
        hit = place[:, j : j + 1] == lane
        found = found + hit.astype(jnp.int32)
        code = code + jnp.where(hit, j * rows + row * sub, 0)
        ids = ids + jnp.where(hit, (row * n + picked) * tiles + block * n + j, 0)
    found = jnp.sum(found, axis=0, keepdims=True)
    code = jnp.where(found > 0, jnp.sum(code, axis=0, keepdims=True), n * rows)
    ids = jnp.where(found > 0, jnp.sum(ids, axis=0, keepdims=True), -1)
    code_ref[...] = jnp.broadcast_to(code, code_ref.shape)
    ids_ref[0] = ids[:, : ids_ref.shape[2]]


def strip_kernel(
    scale, frames, offset, code_ref, part, mine_ref, other_ref, _, out_ref, prod_ref, *last_refs
):
    chips = mine_ref.shape[0]
    n = 2 * chips
    slots = out_ref.shape[0]
    rows = prod_ref.shape[0] // (n + 1)
    sub = rows // n
    groups = LANES // sub
    last = frames // LANES
    gap = frames - last * LANES
    pieces = [part[b * rows : (b + 1) * rows, :] for b in range(last)]
    tail = part[last * rows :, :]
    pieces.append(jnp.concatenate([tail[:, q : q + gap] for q in range(0, LANES, gap)], axis=0))
    left = jnp.concatenate(pieces, axis=1)
    prod_ref[n * rows : n * rows + sub, :] = jnp.zeros((sub, LANES), jnp.float32)
    me = lax.axis_index("row")
    chip, core = me // 2, me % 2
    for m, away in enumerate(aways(chips)):
        pair = jnp.concatenate([mine_ref[m], other_ref[m]], axis=1)
        prod = jnp.dot(left, pair, preferred_element_type=jnp.float32)
        first = lax.rem(chip + (away + chips), chips) * 2
        for h, j in enumerate((first + core, first + 1 - core)):
            at = pl.multiple_of(j * rows, rows)
            prod_ref[pl.ds(at, rows), :] = prod[:, h * LANES : (h + 1) * LANES]
    group = lax.rem(lax.axis_index("col") + (offset + groups), groups)
    into = pl.ds(pl.multiple_of(group * sub, sub), sub)
    for s in range(slots):
        strip = prod_ref[pl.ds(pl.multiple_of(code_ref[0, s], sub), sub), :]
        strip = (strip * scale).astype(jnp.bfloat16)
        if last_refs:
            last_refs[0][s] = strip
        else:
            out_ref[s, into, :] = strip
    if last_refs:
        store = pltpu.make_async_copy(last_refs[0], out_ref.at[:, into, :], last_refs[1])
        store.start()
        store.wait()


def flush_kernel(filled_ref, out_ref, sem):
    store = pltpu.make_async_copy(filled_ref, out_ref, sem)
    store.start()
    store.wait()


def in_vmem(x):
    return pltpu.with_memory_space_constraint(x, pltpu.VMEM)


def in_hbm(x):
    return pltpu.with_memory_space_constraint(x, pltpu.HBM)


def strips(part, offset, code, mine, other, out, scale, final=False):
    chips, frames, _ = mine.shape
    rows = part.shape[0] * LANES // frames
    sub = rows // (2 * chips)
    scratch = [pltpu.VMEM(((2 * chips + 1) * rows, LANES), jnp.float32)]
    if final:
        scratch += [
            pltpu.VMEM((out.shape[0], sub, LANES), out.dtype),
            pltpu.SemaphoreType.DMA,
        ]
    shape, space = (pltpu.HBM, pl.ANY) if final else (pltpu.VMEM, pltpu.VMEM)
    return pl.pallas_call(
        functools.partial(strip_kernel, scale, frames, offset),
        out_shape=shape(out.shape, out.dtype),
        in_specs=[SMEM] + [VMEM] * 3 + [pl.BlockSpec(memory_space=space)],
        out_specs=pl.BlockSpec(memory_space=space),
        input_output_aliases={4: 0},
        scratch_shapes=scratch,
        compiler_params=pltpu.CompilerParams(vmem_limit_bytes=VMEM_LIMIT),
        name="strips",
    )(
        code,
        in_vmem(part),
        in_vmem(mine),
        in_vmem(other),
        in_hbm(out) if final else in_vmem(out),
    )


def aways(chips):
    return [-m for m in range(chips // 2 + 1)] + list(range(1, (chips + 1) // 2))


def stack_kernel(*refs):
    *parts, out_ref = refs
    for m, part in enumerate(parts):
        out_ref[m] = part[...]


def alloc(shape, dtype):
    def nothing(out_ref):
        pass

    return pl.pallas_call(
        nothing,
        out_shape=pltpu.VMEM(shape, dtype),
        out_specs=VMEM,
        compiler_params=pltpu.CompilerParams(vmem_limit_bytes=VMEM_LIMIT),
        name="alloc",
    )()


def gathered(series, keep_mask, row_owner):
    frames = series.shape[0]
    n_row = lax.axis_size("row")
    n_col = lax.axis_size("col")
    row_count, col_count = keep_mask.shape
    slot_limit = max(2, 3 * col_count // 8)
    capacity = row_count * slot_limit
    padded = -(-frames // LANES) * LANES
    groups = n_col // COPIES
    sub = LANES // groups
    bf16 = jnp.bfloat16
    sds = jax.ShapeDtypeStruct

    small = pltpu.CompilerParams(vmem_limit_bytes=VMEM_LIMIT)
    scored, chunks = pl.pallas_call(
        score_kernel,
        out_shape=(pltpu.VMEM((frames, LANES), bf16), pltpu.VMEM((n_col, sub, padded), bf16)),
        in_specs=[VMEM],
        out_specs=(VMEM, VMEM),
        compiler_params=small,
        name="score",
    )(series)

    right = [(i, (i + 2) % n_row) for i in range(n_row)]
    left = [(i, (i - 2) % n_row) for i in range(n_row)]
    swap = [(i, i ^ 1) for i in range(n_row)]
    chips = n_row // 2
    mixed = lax.all_to_all(chunks, "col", 0, 0, tiled=True)
    hops = {"right": [scored], "left": [scored]}

    def hop(way, perm):
        hops[way].append(lax.ppermute(hops[way][-1], "row", perm))

    for step in range(1, chips // 2):
        hop("right", right)
        if step < chips // 2 - 1:
            hop("left", left)
    routed = pl.pallas_call(
        functools.partial(route_kernel, frames),
        out_shape=pltpu.VMEM((n_row, sub, padded), bf16),
        in_specs=[SMEM, VMEM, VMEM],
        out_specs=VMEM,
        compiler_params=small,
        name="route",
    )(in_hbm(row_owner), in_vmem(mixed), in_hbm(keep_mask))
    got = lax.all_to_all(routed, "row", 0, 0, tiled=True)
    long = frames * n_row * sub // LANES
    packed = pl.pallas_call(
        functools.partial(pack_kernel, frames),
        out_shape=pltpu.VMEM((long, LANES), bf16),
        in_specs=[VMEM],
        out_specs=VMEM,
        compiler_params=small,
        name="pack",
    )(in_vmem(got))

    ring_right = [(i, (i + 1) % n_col) for i in range(n_col)]
    ring_left = [(i, (i - 1) % n_col) for i in range(n_col)]
    a = lax.ppermute(packed, "col", ring_right)
    b = lax.ppermute(packed, "col", ring_left)

    code, ids = pl.pallas_call(
        functools.partial(list_kernel, frames),
        out_shape=(
            sds((ALIGN, LANES), jnp.int32),
            sds((1, 1, capacity), jnp.int32),
        ),
        in_specs=[VMEM, VMEM],
        out_specs=(VMEM, VMEM),
        compiler_params=small,
        name="lists",
    )(in_vmem(got), row_owner.reshape(n_row, row_count))

    hops["right"][-1], hops["left"][-1], packed = lax.optimization_barrier(
        (hops["right"][-1], hops["left"][-1], packed)
    )
    hop("right", right)
    hop("left", left)
    mine = pl.pallas_call(
        stack_kernel,
        out_shape=pltpu.VMEM((chips, frames, LANES), bf16),
        in_specs=[VMEM] * chips,
        out_specs=VMEM,
        compiler_params=small,
        name="stack",
    )(*map(in_vmem, hops["right"] + hops["left"][1:]))
    other = lax.ppermute(mine, "row", swap)

    out = alloc((capacity, LANES, LANES), bf16)
    fill = functools.partial(
        strips, code=code, mine=mine, other=other, scale=1.0 / frames
    )
    half = groups // 2
    waiting = [(packed, 0), (a, -1), (b, 1)]
    for step in range(2, half + 1):
        if step > 2:
            out = fill(*waiting.pop(0), out=out)
            a, out = lax.optimization_barrier((a, out))
        a = lax.ppermute(a, "col", ring_right)
        waiting.append((a, -step))
        if step < half:
            if step > 2:
                out = fill(*waiting.pop(0), out=out)
                b, out = lax.optimization_barrier((b, out))
            b = lax.ppermute(b, "col", ring_left)
            waiting.append((b, step))
    for part, offset in sorted(waiting, key=lambda item: item[1] == -half):
        if offset == -half:
            out = pl.pallas_call(
                flush_kernel,
                out_shape=pltpu.HBM(out.shape, out.dtype),
                in_specs=[VMEM],
                out_specs=pl.BlockSpec(memory_space=pl.ANY),
                scratch_shapes=[pltpu.SemaphoreType.DMA],
                compiler_params=small,
                name="flush",
            )(in_vmem(out))
        out = fill(part, offset, out=out, final=offset == -half)
    return out.reshape(1, 1, capacity, LANES, LANES), ids


def solution(mesh):
    in_specs = (P(None, ("subj", "row", "col")), P(("subj", "row"), "col"), P("subj"))
    out_specs = (P(("subj", "row"), "col", None, None, None), P(("subj", "row"), "col", None))
    return jax.shard_map(
        gathered, mesh=mesh, in_specs=in_specs, out_specs=out_specs, check_vma=False
    )
```

```python
import functools

import jax
import jax.numpy as jnp
from jax import lax
from jax.experimental import pallas as pl
from jax.experimental.pallas import tpu as pltpu
from jax.sharding import PartitionSpec as P


EPS = 1e-05
LANES = 128
ALIGN = 8
COPIES = 2
VMEM_LIMIT = 24 * 2**20

VMEM = pl.BlockSpec(memory_space=pltpu.VMEM)
SMEM = pl.BlockSpec(memory_space=pltpu.SMEM)


def score_kernel(series_ref, scored_ref, chunks_ref):
    frames = series_ref.shape[0]
    groups = chunks_ref.shape[0] // COPIES
    sub = LANES // groups
    blocks = frames // LANES
    gap = frames - blocks * LANES
    per = LANES // gap
    x = series_ref[...]
    centred = x - jnp.sum(x, axis=0, keepdims=True) * (1.0 / frames)
    spread = jnp.sum(centred * centred, axis=0, keepdims=True) * (1.0 / frames)
    z = centred * lax.rsqrt(spread + EPS)
    scored_ref[...] = z.astype(jnp.bfloat16)
    for b in range(blocks):
        flipped = z[b * LANES : (b + 1) * LANES].T.astype(jnp.bfloat16)
        flipped = flipped.reshape(groups, sub, LANES)
        for copy in range(COPIES):
            at = copy * groups
            chunks_ref[at : at + groups, b * sub : (b + 1) * sub, :] = flipped
    tail = jnp.concatenate([z[blocks * LANES :], jnp.zeros((LANES - gap, LANES), jnp.float32)])
    tail = tail.T.reshape(groups, sub, LANES)
    few = sub // per
    tail = jnp.concatenate([tail[:, q * few : (q + 1) * few, :gap] for q in range(per)], axis=2)
    spare = chunks_ref.shape[1] - blocks * sub
    tail = jnp.concatenate(
        [tail, jnp.zeros((groups, spare - few, LANES), jnp.float32)], axis=1
    ).astype(jnp.bfloat16)
    for copy in range(COPIES):
        at = copy * groups
        chunks_ref[at : at + groups, blocks * sub :, :] = tail


def route_kernel(spare, owner_ref, chunks_ref, keep_ref, out_ref):
    n, height, _ = chunks_ref.shape
    last = height - ALIGN
    flags = keep_ref[...].astype(jnp.float32)
    flags = jnp.concatenate([flags, jnp.zeros((n, LANES - flags.shape[1]), jnp.float32)], axis=1)
    at_spare = lax.broadcasted_iota(jnp.int32, (ALIGN, LANES), 0) >= ALIGN - spare
    base = lax.axis_index("row") * n
    for k in range(n):
        owner = owner_ref[base + k]
        out_ref[owner, :last, :] = chunks_ref[k, :last, :]
        tail = jnp.where(at_spare, flags[k : k + 1], chunks_ref[k, last:, :].astype(jnp.float32))
        out_ref[owner, last:, :] = tail.astype(jnp.bfloat16)


def pack_kernel(frames, got_ref, packed_ref):
    n = got_ref.shape[0]
    blocks = frames // LANES
    gap = frames - blocks * LANES
    rows = packed_ref.shape[0] * LANES // frames
    sub = rows // n
    for b in range(blocks):
        block = got_ref[:, b * sub : (b + 1) * sub, :]
        packed_ref[b * rows : (b + 1) * rows, :] = block.reshape(rows, LANES)
    per = LANES // gap
    few = sub // per
    tail = got_ref[:, blocks * sub :, :].astype(jnp.float32)[:, :few]
    tail = jnp.concatenate([tail[:, :, q * gap : (q + 1) * gap] for q in range(per)], axis=1)
    tail = tail.reshape(rows, gap)
    depth = rows // per
    tail = jnp.concatenate([tail[q * depth : (q + 1) * depth] for q in range(per)], axis=1)
    packed_ref[blocks * rows :, :] = tail.astype(jnp.bfloat16)


def list_kernel(rows, got_ref, owner_ref, code_ref, ids_ref):
    n, height, _ = got_ref.shape
    sub = rows // n
    me = lax.axis_index("row")
    block = lax.axis_index("col")
    flags = got_ref[:, height - ALIGN :, :].astype(jnp.float32)[:, ALIGN - 1, :n]
    r_of = lax.broadcasted_iota(jnp.int32, (n, n), 0)
    k_of = lax.broadcasted_iota(jnp.int32, (n, n), 1)
    upper = (r_of <= k_of).astype(jnp.float32)
    lower = (r_of > k_of).astype(jnp.float32)
    within = jnp.dot(flags, upper, preferred_element_type=jnp.float32)
    before = jnp.sum(
        jnp.dot(lower, flags, preferred_element_type=jnp.float32), axis=1, keepdims=True
    )
    place = (before + within - 1.0).astype(jnp.int32)
    place = jnp.where(flags > 0.5, place, -1)
    picked = jnp.sum(jnp.where(owner_ref[...] == me, k_of, 0), axis=1, keepdims=True)
    lane = lax.broadcasted_iota(jnp.int32, (n, LANES), 1)
    row = lax.broadcasted_iota(jnp.int32, (n, LANES), 0)
    tiles = n * n
    found = jnp.zeros((n, LANES), jnp.int32)
    code = jnp.zeros((n, LANES), jnp.int32)
    ids = jnp.zeros((n, LANES), jnp.int32)
    for j in range(n):
        hit = place[:, j : j + 1] == lane
        found = found + hit.astype(jnp.int32)
        code = code + jnp.where(hit, j * rows + row * sub, 0)
        ids = ids + jnp.where(hit, (row * n + picked) * tiles + block * n + j, 0)
    found = jnp.sum(found, axis=0, keepdims=True)
    code = jnp.where(found > 0, jnp.sum(code, axis=0, keepdims=True), n * rows)
    ids = jnp.where(found > 0, jnp.sum(ids, axis=0, keepdims=True), -1)
    code_ref[...] = jnp.broadcast_to(code, code_ref.shape)
    ids_ref[0] = ids[:, : ids_ref.shape[2]]


def strip_kernel(
    scale, frames, offset, code_ref, part, mine_ref, other_ref, _, out_ref, prod_ref, *last_refs
):
    chips = mine_ref.shape[0]
    n = 2 * chips
    slots = out_ref.shape[0]
    rows = prod_ref.shape[0] // (n + 1)
    sub = rows // n
    groups = LANES // sub
    last = frames // LANES
    gap = frames - last * LANES
    pieces = [part[b * rows : (b + 1) * rows, :] for b in range(last)]
    tail = part[last * rows :, :]
    pieces.append(jnp.concatenate([tail[:, q : q + gap] for q in range(0, LANES, gap)], axis=0))
    left = jnp.concatenate(pieces, axis=1)
    prod_ref[n * rows : n * rows + sub, :] = jnp.zeros((sub, LANES), jnp.float32)
    me = lax.axis_index("row")
    chip, core = me // 2, me % 2
    for m, away in enumerate(aways(chips)):
        pair = jnp.concatenate([mine_ref[m], other_ref[m]], axis=1)
        prod = jnp.dot(left, pair, preferred_element_type=jnp.float32)
        first = lax.rem(chip + (away + chips), chips) * 2
        for h, j in enumerate((first + core, first + 1 - core)):
            at = pl.multiple_of(j * rows, rows)
            prod_ref[pl.ds(at, rows), :] = prod[:, h * LANES : (h + 1) * LANES]
    group = lax.rem(lax.axis_index("col") + (offset + groups), groups)
    into = pl.ds(pl.multiple_of(group * sub, sub), sub)
    for s in range(slots):
        strip = prod_ref[pl.ds(pl.multiple_of(code_ref[0, s], sub), sub), :]
        strip = (strip * scale).astype(jnp.bfloat16)
        if last_refs:
            last_refs[0][s] = strip
        else:
            out_ref[s, into, :] = strip
    if last_refs:
        store = pltpu.make_async_copy(last_refs[0], out_ref.at[:, into, :], last_refs[1])
        store.start()
        store.wait()


def flush_kernel(filled_ref, out_ref, sem):
    store = pltpu.make_async_copy(filled_ref, out_ref, sem)
    store.start()
    store.wait()


def in_vmem(x):
    return pltpu.with_memory_space_constraint(x, pltpu.VMEM)


def in_hbm(x):
    return pltpu.with_memory_space_constraint(x, pltpu.HBM)


def strips(part, offset, code, mine, other, out, scale, final=False):
    chips, frames, _ = mine.shape
    rows = part.shape[0] * LANES // frames
    sub = rows // (2 * chips)
    scratch = [pltpu.VMEM(((2 * chips + 1) * rows, LANES), jnp.float32)]
    if final:
        scratch += [
            pltpu.VMEM((out.shape[0], sub, LANES), out.dtype),
            pltpu.SemaphoreType.DMA,
        ]
    shape, space = (pltpu.HBM, pl.ANY) if final else (pltpu.VMEM, pltpu.VMEM)
    return pl.pallas_call(
        functools.partial(strip_kernel, scale, frames, offset),
        out_shape=shape(out.shape, out.dtype),
        in_specs=[SMEM] + [VMEM] * 3 + [pl.BlockSpec(memory_space=space)],
        out_specs=pl.BlockSpec(memory_space=space),
        input_output_aliases={4: 0},
        scratch_shapes=scratch,
        compiler_params=pltpu.CompilerParams(vmem_limit_bytes=VMEM_LIMIT),
        name="strips",
    )(
        code,
        in_vmem(part),
        in_vmem(mine),
        in_vmem(other),
        in_hbm(out) if final else in_vmem(out),
    )


def aways(chips):
    return [-m for m in range(chips // 2 + 1)] + list(range(1, (chips + 1) // 2))


def stack_kernel(*refs):
    *parts, out_ref = refs
    for m, part in enumerate(parts):
        out_ref[m] = part[...]


def alloc(shape, dtype):
    def nothing(out_ref):
        pass

    return pl.pallas_call(
        nothing,
        out_shape=pltpu.VMEM(shape, dtype),
        out_specs=VMEM,
        compiler_params=pltpu.CompilerParams(vmem_limit_bytes=VMEM_LIMIT),
        name="alloc",
    )()


def gathered(series, keep_mask, row_owner):
    frames = series.shape[0]
    n_row = lax.axis_size("row")
    n_col = lax.axis_size("col")
    row_count, col_count = keep_mask.shape
    slot_limit = max(2, 3 * col_count // 8)
    capacity = row_count * slot_limit
    groups = n_col // COPIES
    sub = LANES // groups
    used = frames * sub // LANES
    height = (used // ALIGN + 1) * ALIGN
    bf16 = jnp.bfloat16
    sds = jax.ShapeDtypeStruct

    small = pltpu.CompilerParams(vmem_limit_bytes=VMEM_LIMIT)
    scored, chunks = pl.pallas_call(
        score_kernel,
        out_shape=(pltpu.VMEM((frames, LANES), bf16), pltpu.VMEM((n_col, height, LANES), bf16)),
        in_specs=[VMEM],
        out_specs=(VMEM, VMEM),
        compiler_params=small,
        name="score",
    )(series)

    right = [(i, (i + 2) % n_row) for i in range(n_row)]
    left = [(i, (i - 2) % n_row) for i in range(n_row)]
    swap = [(i, i ^ 1) for i in range(n_row)]
    chips = n_row // 2
    mixed = lax.all_to_all(chunks, "col", 0, 0, tiled=True)
    hops = {"right": [scored], "left": [scored]}

    def hop(way, perm):
        hops[way].append(lax.ppermute(hops[way][-1], "row", perm))

    for step in range(1, chips // 2):
        hop("right", right)
        if step < chips // 2 - 1:
            hop("left", left)
    routed = pl.pallas_call(
        functools.partial(route_kernel, height - used),
        out_shape=pltpu.VMEM((n_row, height, LANES), bf16),
        in_specs=[SMEM, VMEM, VMEM],
        out_specs=VMEM,
        compiler_params=small,
        name="route",
    )(in_hbm(row_owner), in_vmem(mixed), in_hbm(keep_mask))
    got = lax.all_to_all(routed, "row", 0, 0, tiled=True)
    long = frames * n_row * sub // LANES
    packed = pl.pallas_call(
        functools.partial(pack_kernel, frames),
        out_shape=pltpu.VMEM((long, LANES), bf16),
        in_specs=[VMEM],
        out_specs=VMEM,
        compiler_params=small,
        name="pack",
    )(in_vmem(got))

    ring_right = [(i, (i + 1) % n_col) for i in range(n_col)]
    ring_left = [(i, (i - 1) % n_col) for i in range(n_col)]
    a = lax.ppermute(packed, "col", ring_right)
    b = lax.ppermute(packed, "col", ring_left)

    code, ids = pl.pallas_call(
        functools.partial(list_kernel, n_row * sub),
        out_shape=(
            sds((ALIGN, LANES), jnp.int32),
            sds((1, 1, capacity), jnp.int32),
        ),
        in_specs=[VMEM, VMEM],
        out_specs=(VMEM, VMEM),
        compiler_params=small,
        name="lists",
    )(in_vmem(got), row_owner.reshape(n_row, row_count))

    hops["right"][-1], hops["left"][-1], packed = lax.optimization_barrier(
        (hops["right"][-1], hops["left"][-1], packed)
    )
    hop("right", right)
    hop("left", left)
    mine = pl.pallas_call(
        stack_kernel,
        out_shape=pltpu.VMEM((chips, frames, LANES), bf16),
        in_specs=[VMEM] * chips,
        out_specs=VMEM,
        compiler_params=small,
        name="stack",
    )(*map(in_vmem, hops["right"] + hops["left"][1:]))
    other = lax.ppermute(mine, "row", swap)

    out = alloc((capacity, LANES, LANES), bf16)
    fill = functools.partial(
        strips, code=code, mine=mine, other=other, scale=1.0 / frames
    )
    half = groups // 2
    waiting = [(packed, 0), (a, -1), (b, 1)]
    for step in range(2, half + 1):
        if step > 2:
            out = fill(*waiting.pop(0), out=out)
            a, out = lax.optimization_barrier((a, out))
        a = lax.ppermute(a, "col", ring_right)
        waiting.append((a, -step))
        if step < half:
            if step > 2:
                out = fill(*waiting.pop(0), out=out)
                b, out = lax.optimization_barrier((b, out))
            b = lax.ppermute(b, "col", ring_left)
            waiting.append((b, step))
    for part, offset in sorted(waiting, key=lambda item: item[1] == -half):
        if offset == -half:
            out = pl.pallas_call(
                flush_kernel,
                out_shape=pltpu.HBM(out.shape, out.dtype),
                in_specs=[VMEM],
                out_specs=pl.BlockSpec(memory_space=pl.ANY),
                scratch_shapes=[pltpu.SemaphoreType.DMA],
                compiler_params=small,
                name="flush",
            )(in_vmem(out))
        out = fill(part, offset, out=out, final=offset == -half)
    return out.reshape(1, 1, capacity, LANES, LANES), ids


def solution(mesh):
    in_specs = (P(None, ("subj", "row", "col")), P(("subj", "row"), "col"), P("subj"))
    out_specs = (P(("subj", "row"), "col", None, None, None), P(("subj", "row"), "col", None))
    return jax.shard_map(
        gathered, mesh=mesh, in_specs=in_specs, out_specs=out_specs, check_vma=False
    )
```
